1024 devices in a mesh: replica: 16 (over z, core), fsdp: 64 (over x, y).
Axes of the slice: x: 8, y: 8, z: 8, core: 2. Of those that a mesh axis runs over, the one named last changes fastest.
Arguments:
- states: bfloat16 [1024, 256, 2048], P(('replica', 'fsdp'))
- cotangent: bfloat16 [1024, 256, 512], P(('replica', 'fsdp')), may hold values from -6 to 6
- kv_weight: bfloat16 [2048, 512], P('fsdp'), may hold values from -0.125 to 0.125
- norm_gain: bfloat16 [2048], P('fsdp'), may hold values from -1.5 to 1.5
- prompt_len: int32 [1024], P(('replica', 'fsdp')), may hold values from 1 to 255, as said below
- response_len: int32 [1024], P(('replica', 'fsdp')), may hold values from 1 to 192
- reward_bucket: int32 [1024], P(('replica', 'fsdp')), may hold values from 0 to 10, as said below
Outputs:
- key_values: bfloat16 [1024, 256, 512], P(('replica', 'fsdp'))
- grad_weight: float32 [2048, 512], P('fsdp')
- grad_gain: float32 [2048], P('fsdp')
The draws below stay inside these ranges and needn't reach their ends.
Inputs may be any that keep to these rules, and one draw needn't show every extreme that they name: prompt_len + response_len <= 256 for every rollout. `reward_bucket`: some rollout has level 0 and some has level 10.
All inputs are finite; a program needn't handle non-finite values.
Results may differ from the reference program's by a relative error of at most 0.005.
Values may be sent and summed in bfloat16 or wider, within the bound.
No kernel may reach another device: no remote copies, remote signals or barrier semaphores. Data moves between devices by JAX's collectives and lax.ppermute only.
A program may use at most 64 MiB of HBM per device.

```python
import math
import jax
import jax.numpy as jnp
from jax import lax

D = 2048
KV = 512
SEQ = 256
BUCKETS = 11
ROLLOUTS = 1024


def lengths_pair(key):
    salted = jax.random.fold_in(key, 101)
    key_length, key_prompt = jax.random.split(salted)
    rollout_index = jnp.arange(ROLLOUTS, dtype=jnp.int32)
    ceiling = SEQ // 4 + SEQ // 2 * rollout_index // max(ROLLOUTS - 1, 1)
    response = 1 + jax.random.randint(key_length, (ROLLOUTS,), 0, ceiling, dtype=jnp.int32)
    response = response.at[ROLLOUTS - 1].set(SEQ // 4 + SEQ // 2).at[0].set(1)
    prompt = 1 + jax.random.randint(key_prompt, (ROLLOUTS,), 0, SEQ - response, dtype=jnp.int32)
    prompt = prompt.at[0].set(SEQ - 1)
    return (prompt, response)


def draw_prompt_len(key, part):
    return lengths_pair(key)[0]


def draw_response_len(key, part):
    return lengths_pair(key)[1]


def draw_reward_bucket(key, part):
    salted = jax.random.fold_in(key, 202)
    rollout_index = jnp.arange(ROLLOUTS, dtype=jnp.int32)
    ceiling = BUCKETS // 3 + (BUCKETS - BUCKETS // 3) * rollout_index // max(ROLLOUTS - 1, 1)
    levels = jax.random.randint(salted, (ROLLOUTS,), 0, ceiling, dtype=jnp.int32)
    return levels.at[0].set(0).at[ROLLOUTS - 1].set(BUCKETS - 1)


def draw_states(key, part):
    salted = jax.random.fold_in(key, 303)
    key_base, key_rows, key_columns = jax.random.split(salted, 3)
    base = jax.random.normal(key_base, (ROLLOUTS, SEQ, D), jnp.float32)
    row_scale = jnp.exp(jax.random.uniform(key_rows, (ROLLOUTS, SEQ, 1), jnp.float32, math.log(0.3), math.log(3.0)))
    column_scale = jnp.exp(jax.random.uniform(key_columns, (1, 1, D), jnp.float32, math.log(0.3), math.log(3.0)))
    return (base * row_scale * column_scale).astype(jnp.bfloat16)


def steps_of(own_key, extent, cuts, smallest, largest):
    factor_of = 1.0
    for dim, blocks in cuts:
        steps = jax.random.uniform(jax.random.fold_in(jax.random.fold_in(own_key, 6), dim), (blocks,), jnp.float32, smallest / len(cuts), largest / len(cuts))
        factor_of = factor_of * jnp.repeat(jnp.exp(steps), extent[dim] // blocks).reshape((-1,) + (1,) * (len(extent) - 1 - dim))
    return factor_of


def scatter_about(rng, extent, deviation, most, cuts=(), kind=jnp.bfloat16):
    array = deviation * jax.random.normal(rng, extent, jnp.float32)
    if cuts:
        array = array * steps_of(rng, extent, cuts, -0.22, 0.18)
    return jnp.clip(array, -most, most).astype(kind)


def setup_inputs(seed: int = 0) -> dict:
    arg_keys = jax.random.split(jax.random.key(seed), 8)
    return {
        "states": draw_states(jax.random.fold_in(arg_keys[7], 71), 0),
        "cotangent": scatter_about(arg_keys[1], (ROLLOUTS, SEQ, KV), 1.0, 6.0, ((0, 1024),)),
        "kv_weight": scatter_about(arg_keys[2], (D, KV), D ** -0.5, 0.125, ((0, 64),)),
        "norm_gain": scatter_about(arg_keys[3], (D,), 0.3, 1.5, ((0, 64),)),
        "prompt_len": draw_prompt_len(jax.random.fold_in(arg_keys[7], 71), 0),
        "response_len": draw_response_len(jax.random.fold_in(arg_keys[7], 71), 0),
        "reward_bucket": draw_reward_bucket(jax.random.fold_in(arg_keys[7], 71), 0),
    }


EPSILON = 1e-06

def reference(states, cotangent, kv_weight, norm_gain, prompt_len, response_len, reward_bucket):
    rollout_count = states.shape[0]
    seq_rows = states.shape[1]
    width = states.shape[2]
    feature_count = kv_weight.shape[1]
    reward_value = reward_bucket.astype(jnp.float32)
    token_total = jnp.sum(response_len.astype(jnp.float32))
    average = jnp.sum(reward_value) / rollout_count
    variance = jnp.sum(reward_value * reward_value) / rollout_count - average * average
    grad_scale = lax.rsqrt(variance + EPSILON) * lax.rsqrt(token_total)
    gain_wide = norm_gain.astype(jnp.float32)
    position = jnp.arange(seq_rows, dtype=jnp.int32)
    group_size = math.gcd(rollout_count, 64)
    group_count = rollout_count // group_size

    def one_group(totals, pieces):
        grad_weight, grad_gain = totals
        part_states, part_cotangent, part_prompt, part_response, part_reward = pieces
        widened = part_states.astype(jnp.float32)
        unit_rows = widened * lax.rsqrt(lax.optimization_barrier(jnp.mean(widened * widened, axis=-1, keepdims=True)) + EPSILON)
        normed = (unit_rows * (1.0 + gain_wide)).astype(jnp.bfloat16)
        flat_normed = normed.reshape(-1, width)
        key_values = jnp.dot(flat_normed, kv_weight, preferred_element_type=jnp.float32).astype(jnp.bfloat16)
        live_flag = (position[None, :] >= part_prompt[:, None]) & (position[None, :] < part_prompt[:, None] + part_response[:, None])
        coefficient = live_flag.astype(jnp.float32) * (part_reward - average)[:, None] * grad_scale
        weighted = (coefficient[:, :, None] * part_cotangent.astype(jnp.float32)).astype(jnp.bfloat16)
        flat_weighted = weighted.reshape(-1, feature_count)
        grad_weight = grad_weight + jnp.dot(flat_normed.T, flat_weighted, preferred_element_type=jnp.float32)
        backward = jnp.dot(flat_weighted, kv_weight.T, preferred_element_type=jnp.float32)
        grad_gain = grad_gain + lax.optimization_barrier(jnp.sum(unit_rows.reshape(-1, width) * backward, axis=0))
        return ((grad_weight, grad_gain), key_values.reshape(group_size, seq_rows, feature_count))
    start_totals = (jnp.zeros((width, feature_count), jnp.float32), jnp.zeros((width,), jnp.float32))
    grouped = (states.reshape(group_count, group_size, seq_rows, width), cotangent.reshape(group_count, group_size, seq_rows, feature_count), prompt_len.reshape(group_count, group_size), response_len.reshape(group_count, group_size), reward_value.reshape(group_count, group_size))
    (grad_weight, grad_gain), key_values = lax.scan(one_group, start_totals, grouped)
    return (key_values.reshape(rollout_count, seq_rows, feature_count), grad_weight, grad_gain)
```

```python
import jax
import jax.numpy as jnp
from jax import lax
from jax.sharding import Mesh
from jax.sharding import PartitionSpec as P

CORE, Z, X, Y = "core", "z", "x", "y"
REPLICA = (Z, CORE)
FSDP = (X, Y)
ALL = (Z, CORE, X, Y)
EPSILON = 1e-06


def from_all(value, axes):
    count = lax.axis_size(axes)
    copies = jnp.broadcast_to(value[None], (count, *value.shape))
    return lax.all_to_all(copies, axes, 0, 0, tiled=True)


def shards(states, cotangent, kv_weight, norm_gain, prompt_len, response_len, reward_bucket):
    fsdp, replicas = lax.axis_size(FSDP), lax.axis_size(REPLICA)
    rows_own, features = kv_weight.shape
    rows_half = rows_own // 2
    seq, width = states.shape[1:]
    weight_full = lax.all_gather(kv_weight, FSDP, axis=0, tiled=True)

    reward = reward_bucket.astype(jnp.float32)
    stats = jnp.concatenate([reward, reward * reward, response_len.astype(jnp.float32)])
    stats = from_all(jnp.pad(stats, (0, 125)), REPLICA).sum(axis=0)[:3]
    gain_own = norm_gain.astype(jnp.float32)
    mixed = jnp.concatenate([gain_own, stats, jnp.zeros((128 - rows_own - 3,), jnp.float32)])
    mixed = from_all(mixed, FSDP)
    gain_full = mixed[:, :rows_own].reshape(width)
    reward_sum, square_sum, token_total = mixed[:, rows_own : rows_own + 3].sum(axis=0)
    count = fsdp * replicas
    average = reward_sum / count
    variance = square_sum / count - average * average
    grad_scale = lax.rsqrt(variance + EPSILON) * lax.rsqrt(token_total)
    scale_own = (reward[0] - average) * grad_scale

    widened = states[0].astype(jnp.float32)
    unit = widened * lax.rsqrt(jnp.mean(widened * widened, axis=-1, keepdims=True) + EPSILON)
    position = jnp.arange(seq, dtype=jnp.int32)
    live = (position >= prompt_len[0]) & (position < prompt_len[0] + response_len[0])
    masked = jnp.where(live[:, None], cotangent[0], jnp.zeros((), cotangent.dtype))
    product = jnp.einsum(
        "td,tk->dk", unit.astype(jnp.bfloat16), masked, preferred_element_type=jnp.float32
    )
    scaled = (product * scale_own).astype(jnp.bfloat16)
    halves = scaled.reshape(fsdp, 2, rows_half, features)
    halves = halves.transpose(1, 0, 2, 3)

    pair = lax.all_to_all(halves, CORE, 0, 0, tiled=True)
    chip = pair.astype(jnp.float32).sum(axis=0).astype(jnp.bfloat16)
    plane = lax.all_to_all(chip, FSDP, 0, 0, tiled=True)
    plane = plane.astype(jnp.float32).sum(axis=0)
    every = from_all(plane, REPLICA).reshape(replicas // 2, 2, rows_half, features)
    total = every.sum(axis=0).reshape(rows_own, features)

    grad_weight = total * (1.0 + gain_own)[:, None]
    grad_gain = jnp.sum(total * kv_weight.astype(jnp.float32), axis=1)

    normed = (unit * (1.0 + gain_full)).astype(jnp.bfloat16)
    key_values = jnp.dot(normed, weight_full, preferred_element_type=jnp.float32)
    return (key_values.astype(jnp.bfloat16)[None], grad_weight, grad_gain)


def solution(mesh):
    torus = Mesh(mesh.devices.reshape(8, 2, 8, 8), ALL)
    split = (Z, CORE, X, Y)
    return jax.shard_map(
        shards,
        mesh=torus,
        in_specs=(
            P(split, None, None),
            P(split, None, None),
            P(FSDP, None),
            P(FSDP),
            P(split),
            P(split),
            P(split),
        ),
        out_specs=(P(split, None, None), P(FSDP, None), P(FSDP)),
        check_vma=False,
    )
```

```python
import jax
import jax.numpy as jnp
from jax import lax
from jax.sharding import Mesh
from jax.sharding import PartitionSpec as P

CORE, Z, X, Y = "core", "z", "x", "y"
REPLICA = (Z, CORE)
FSDP = (X, Y)
ALL = (Z, CORE, X, Y)
EPSILON = 1e-06
SWAP = ((0, 1), (1, 0))
LANES = 128
DIGIT = 64.0


def from_all(value, axes):
    count = lax.axis_size(axes)
    copies = jnp.broadcast_to(value[None], (count, *value.shape))
    return lax.all_to_all(copies, axes, 0, 0, tiled=True)


def half_of(value, which):
    half = value.shape[-1] // 2
    return lax.dynamic_slice_in_dim(value, which * half, half, value.ndim - 1)


def side_by_side(mine, other, core):
    left = jnp.where(core == 0, mine, other)
    right = jnp.where(core == 0, other, mine)
    return jnp.concatenate([left, right], axis=-1)


def shards(states, cotangent, kv_weight, norm_gain, prompt_len, response_len, reward_bucket):
    fsdp, replicas = lax.axis_size(FSDP), lax.axis_size(REPLICA)
    core = lax.axis_index(CORE)
    rows_own, features = kv_weight.shape
    seq, width = states.shape[1:]
    with jax.named_scope("column"):
        reward = reward_bucket.astype(jnp.float32)
        stats = jnp.concatenate([reward, reward * reward, response_len.astype(jnp.float32)])
        stats = from_all(jnp.pad(stats, (0, LANES - 3)), REPLICA)
    reward_other = stats[2 * lax.axis_index(Z) + 1 - core, 0]
    stats = stats.sum(axis=0)
    square_high, token_high = jnp.floor(stats[1:3] / DIGIT)
    square_low, token_low = stats[1] - DIGIT * square_high, stats[2] - DIGIT * token_high
    digits = jnp.stack([stats[0], square_high, square_low, token_high, token_low])
    tail = jnp.concatenate([norm_gain, digits.astype(jnp.bfloat16)])
    tail = jnp.pad(tail, (0, LANES - tail.shape[0]))[None]
    weight_own = half_of(kv_weight, core)
    lane_tiles = weight_own.shape[-1] // LANES
    weight_own = [weight_own[:, k * LANES : (k + 1) * LANES] for k in range(lane_tiles)]
    with jax.named_scope("weight"):
        filled = from_all(jnp.concatenate([*weight_own, tail]), FSDP)
    weight_mine = jnp.concatenate(
        [
            filled[:, k * rows_own : (k + 1) * rows_own].reshape(width, LANES)
            for k in range(lane_tiles)
        ],
        axis=-1,
    )
    filled = filled[:, lane_tiles * rows_own].astype(jnp.float32)
    gain_own = norm_gain.astype(jnp.float32)
    gain_full = filled[:, :rows_own].reshape(width)
    digits = filled[:, rows_own : rows_own + 5].sum(axis=0)
    count = fsdp * replicas
    average = digits[0] / count
    variance = (DIGIT * digits[1] + digits[2]) / count - average * average
    token_total = DIGIT * digits[3] + digits[4]
    grad_scale = lax.rsqrt(variance + EPSILON) * lax.rsqrt(token_total)

    widened = states[0].astype(jnp.float32)
    unit = widened * lax.rsqrt(jnp.mean(widened * widened, axis=-1, keepdims=True) + EPSILON)
    coarse = lax.reduce_precision(unit, 8, 7)
    fine = (unit - coarse).astype(jnp.bfloat16)
    coarse = coarse.astype(jnp.bfloat16)
    position = jnp.arange(seq, dtype=jnp.int32)
    live = (position >= prompt_len[0]) & (position < prompt_len[0] + response_len[0])
    masked = jnp.where(live[:, None], cotangent[0], jnp.zeros((), cotangent.dtype))

    def product(part):
        def with_unit(rows):
            return jnp.einsum("td,tk->dk", rows, part, preferred_element_type=jnp.float32)

        return with_unit(coarse) + with_unit(fine)

    sent = product(half_of(masked, 1 - core)).astype(jnp.bfloat16)
    got = lax.ppermute(sent, CORE, SWAP)
    kept = lax.optimization_barrier(product(half_of(masked, core)))

    chip = (reward[0] - average) * kept + (reward_other - average) * got.astype(jnp.float32)
    chip = chip.astype(jnp.bfloat16).reshape(fsdp, rows_own, features // 2)
    plane = lax.all_to_all(chip, FSDP, 0, 0, tiled=True)
    plane = plane.astype(jnp.float32).sum(axis=0)
    mine = from_all(plane, Z).sum(axis=0) * grad_scale
    total = side_by_side(mine, lax.ppermute(mine, CORE, SWAP), core)

    grad_weight = total * (1.0 + gain_own)[:, None]
    grad_gain = jnp.sum(total * kv_weight.astype(jnp.float32), axis=1)

    normed = (unit * (1.0 + gain_full)).astype(jnp.bfloat16)
    weight_other = lax.ppermute(weight_mine, CORE, SWAP)

    def projected(weight):
        result = jnp.dot(normed, weight, preferred_element_type=jnp.float32)
        return result.astype(jnp.bfloat16)

    key_values = side_by_side(projected(weight_mine), projected(weight_other), core)
    return (key_values[None], grad_weight, grad_gain)


def solution(mesh):
    torus = Mesh(mesh.devices.reshape(8, 2, 8, 8), ALL)
    return jax.shard_map(
        shards,
        mesh=torus,
        in_specs=(
            P(ALL, None, None),
            P(ALL, None, None),
            P(FSDP, None),
            P(FSDP),
            P(ALL),
            P(ALL),
            P(ALL),
        ),
        out_specs=(P(ALL, None, None), P(FSDP, None), P(FSDP)),
        check_vma=False,
    )
```

```python
import jax
import jax.numpy as jnp
from jax import lax
from jax.sharding import Mesh
from jax.sharding import PartitionSpec as P

CORE, Z, X, Y = "core", "z", "x", "y"
REPLICA = (Z, CORE)
FSDP = (X, Y)
ALL = (Z, CORE, X, Y)
EPSILON = 1e-06
GROUP = 4
LANES = 128
DIGIT = 64.0


def from_all(value, axes):
    count = lax.axis_size(axes)
    copies = jnp.broadcast_to(value[None], (count, *value.shape))
    return lax.all_to_all(copies, axes, 0, 0, tiled=True)


def to_peer(value, flip):
    count = lax.axis_size(REPLICA)
    return lax.ppermute(value, REPLICA, [(i, i ^ flip) for i in range(count)])


def shards(states, cotangent, kv_weight, norm_gain, prompt_len, response_len, reward_bucket):
    fsdp, replicas = lax.axis_size(FSDP), lax.axis_size(REPLICA)
    member = lax.axis_index(REPLICA)
    place = member % GROUP
    rows_own, features = kv_weight.shape
    quarter = features // GROUP
    seq, width = states.shape[1:]

    def quarter_of(value, flip):
        return lax.dynamic_slice_in_dim(value, (place ^ flip) * quarter, quarter, value.ndim - 1)

    with jax.named_scope("column"):
        reward = reward_bucket.astype(jnp.float32)
        stats = jnp.concatenate([reward, reward * reward, response_len.astype(jnp.float32)])
        stats = from_all(jnp.pad(stats, (0, LANES - 3)), REPLICA)
    others = jnp.arange(replicas)
    rewards = jnp.stack(
        [jnp.sum(jnp.where(others == member ^ flip, stats[:, 0], 0.0)) for flip in range(GROUP)]
    )
    sums = stats.sum(axis=0)
    high = jnp.floor(sums / DIGIT)
    low = sums - DIGIT * high
    extra = jnp.stack([jnp.pad(norm_gain, (0, LANES - rows_own)), high.astype(jnp.bfloat16), low.astype(jnp.bfloat16)])
    with jax.named_scope("weight"):
        filled = from_all(jnp.concatenate([quarter_of(kv_weight, 0), extra]), FSDP)
    weights = [filled[:, :rows_own].reshape(width, quarter)]
    extra = filled[:, rows_own:].astype(jnp.float32)
    gain_own = norm_gain.astype(jnp.float32)
    gain_full = extra[:, 0, :rows_own].reshape(width)
    sums = jnp.sum(DIGIT * extra[:, 1] + extra[:, 2], axis=0)
    count = fsdp * replicas
    average = sums[0] / count
    variance = sums[1] / count - average * average
    grad_scale = lax.rsqrt(variance + EPSILON) * lax.rsqrt(sums[2])

    with jax.named_scope("local"):
        widened = states[0].astype(jnp.float32)
        mean = jnp.mean(widened * widened, axis=-1, keepdims=True)
        unit = widened * lax.rsqrt(mean + EPSILON)
        coarse = lax.reduce_precision(unit, 8, 7)
        fine = (unit - coarse).astype(jnp.bfloat16)
        coarse = coarse.astype(jnp.bfloat16)
        position = jnp.arange(seq, dtype=jnp.int32)
        live = (position >= prompt_len[0]) & (position < prompt_len[0] + response_len[0])
        masked = jnp.where(live[:, None], cotangent[0], jnp.zeros((), cotangent.dtype))

    def product(flip):
        def with_unit(rows):
            part = quarter_of(masked, flip)
            return jnp.einsum("td,tk->dk", rows, part, preferred_element_type=jnp.float32)

        return with_unit(coarse) + with_unit(fine)

    got = {}
    for flip in (3, 2, 1):
        with jax.named_scope(f"peer{flip}"):
            got[flip] = to_peer(product(flip).astype(jnp.bfloat16), flip)
    with jax.named_scope("kept"):
        got[0] = lax.optimization_barrier(product(0))

    scales = rewards - average
    chip = sum(scales[flip] * got[flip].astype(jnp.float32) for flip in range(GROUP))
    chip = chip.astype(jnp.bfloat16).reshape(fsdp, rows_own, quarter)
    with jax.named_scope("plane"):
        plane = lax.all_to_all(chip, FSDP, 0, 0, tiled=True)
    plane = plane.astype(jnp.float32).sum(axis=0)
    with jax.named_scope("last"):
        every = from_all(plane, REPLICA)
    every = every.reshape(replicas // GROUP, GROUP, rows_own, quarter).sum(axis=0)
    total = jnp.concatenate([every[k] for k in range(GROUP)], axis=-1) * grad_scale

    grad_weight = total * (1.0 + gain_own)[:, None]
    grad_gain = jnp.sum(total * kv_weight.astype(jnp.float32), axis=1)

    with jax.named_scope("weight2"):
        weights.append(to_peer(weights[0], 1))
        weights.append(to_peer(weights[0], 2))
    with jax.named_scope("weight3"):
        weights.append(to_peer(weights[2], 1))
    normed = (unit * (1.0 + gain_full)).astype(jnp.bfloat16)
    parts = [
        jnp.dot(normed, w, preferred_element_type=jnp.float32).astype(jnp.bfloat16) for w in weights
    ]
    placed = []
    for k in range(GROUP):
        chosen = parts[0]
        for flip in range(1, GROUP):
            chosen = jnp.where(place ^ flip == k, parts[flip], chosen)
        placed.append(chosen)
    key_values = jnp.concatenate(placed, axis=-1)
    return (key_values[None], grad_weight, grad_gain)


def solution(mesh):
    torus = Mesh(mesh.devices.reshape(8, 2, 8, 8), ALL)
    return jax.shard_map(
        shards,
        mesh=torus,
        in_specs=(
            P(ALL, None, None),
            P(ALL, None, None),
            P(FSDP, None),
            P(FSDP),
            P(ALL),
            P(ALL),
            P(ALL),
        ),
        out_specs=(P(ALL, None, None), P(FSDP, None), P(FSDP)),
        check_vma=False,
    )
```

```python
import functools

import jax
import jax.numpy as jnp
from jax import lax
from jax.experimental import pallas as pl
from jax.experimental.pallas import tpu as pltpu
from jax.sharding import Mesh
from jax.sharding import PartitionSpec as P

CORE, Z, X, Y = "core", "z", "x", "y"
REPLICA = (Z, CORE)
FSDP = (X, Y)
ALL = (Z, CORE, X, Y)
EPSILON = 1e-06
GROUP = 4
LANES = 128
DIGIT = 64.0
STEP = 128


def from_all(value, axes):
    count = lax.axis_size(axes)
    copies = jnp.broadcast_to(value[None], (count, *value.shape))
    return lax.all_to_all(copies, axes, 0, 0, tiled=True)


def to_peer(value, flip):
    count = lax.axis_size(REPLICA)
    return lax.ppermute(value, REPLICA, [(i, i ^ flip) for i in range(count)])


def combine(count, rewards_ref, filled_ref, kept_ref, *refs):
    *got_refs, out_ref = refs
    width, _ = out_ref.shape
    extra_rows = filled_ref.shape[1] - 3
    digits = filled_ref[:, extra_rows:, :].astype(jnp.float32).sum(axis=0)
    sums = DIGIT * digits[1:2] + digits[2:3]
    average = sums[0, 0] / count
    scales = [rewards_ref[flip] - average for flip in range(GROUP)]

    def block(step, carry):
        rows = pl.ds(step * STEP, STEP)
        chip = scales[0] * kept_ref[rows, :]
        for flip in range(1, GROUP):
            chip += scales[flip] * got_refs[flip - 1][rows, :].astype(jnp.float32)
        out_ref[rows, :] = chip.astype(out_ref.dtype)
        return carry

    lax.fori_loop(0, width // STEP, block, 0)


def combined(rewards, filled, parts, count):
    width, quarter = parts[0].shape
    vmem = pl.BlockSpec(memory_space=pltpu.VMEM)
    return pl.pallas_call(
        functools.partial(combine, count),
        out_shape=jax.ShapeDtypeStruct((width, quarter), jnp.bfloat16),
        in_specs=[pl.BlockSpec(memory_space=pltpu.SMEM), *([vmem] * (1 + GROUP))],
        out_specs=vmem,
        compiler_params=pltpu.CompilerParams(vmem_limit_bytes=16 * 2**20),
        cost_estimate=pl.CostEstimate(
            flops=8 * width * quarter, bytes_accessed=12 * width * quarter, transcendentals=0
        ),
        name="combine",
    )(rewards, filled, *parts)


def shards(states, cotangent, kv_weight, norm_gain, prompt_len, response_len, reward_bucket):
    fsdp, replicas = lax.axis_size(FSDP), lax.axis_size(REPLICA)
    member = lax.axis_index(REPLICA)
    place = member % GROUP
    rows_own, features = kv_weight.shape
    quarter = features // GROUP
    seq, width = states.shape[1:]

    def quarter_of(value, flip):
        return lax.dynamic_slice_in_dim(value, (place ^ flip) * quarter, quarter, value.ndim - 1)

    reward = reward_bucket.astype(jnp.float32)
    stats = jnp.concatenate([reward, reward * reward, response_len.astype(jnp.float32)])
    stats = from_all(jnp.pad(stats, (0, LANES - 3)), REPLICA)
    others = jnp.arange(replicas)
    rewards = jnp.stack(
        [jnp.sum(jnp.where(others == member ^ flip, stats[:, 0], 0.0)) for flip in range(GROUP)]
    )
    sums = stats.sum(axis=0)
    high = jnp.floor(sums / DIGIT)
    low = sums - DIGIT * high
    extra = jnp.stack([jnp.pad(norm_gain, (0, LANES - rows_own)), high.astype(jnp.bfloat16), low.astype(jnp.bfloat16)])
    filled = from_all(jnp.concatenate([quarter_of(kv_weight, 0), extra]), FSDP)
    weights = [filled[:, :rows_own].reshape(width, quarter)]
    extra = filled[:, rows_own:].astype(jnp.float32)
    gain_own = norm_gain.astype(jnp.float32)
    gain_full = extra[:, 0, :rows_own].reshape(width)
    sums = jnp.sum(DIGIT * extra[:, 1] + extra[:, 2], axis=0)
    count = fsdp * replicas
    average = sums[0] / count
    variance = sums[1] / count - average * average
    grad_scale = lax.rsqrt(variance + EPSILON) * lax.rsqrt(sums[2])

    widened = states[0].astype(jnp.float32)
    mean = jnp.mean(widened * widened, axis=-1, keepdims=True)
    unit = widened * lax.rsqrt(mean + EPSILON)
    coarse = lax.reduce_precision(unit, 8, 7)
    fine = (unit - coarse).astype(jnp.bfloat16)
    coarse = coarse.astype(jnp.bfloat16)
    position = jnp.arange(seq, dtype=jnp.int32)
    live = (position >= prompt_len[0]) & (position < prompt_len[0] + response_len[0])
    masked = jnp.where(live[:, None], cotangent[0], jnp.zeros((), cotangent.dtype))

    def product(flip):
        def with_unit(rows):
            part = quarter_of(masked, flip)
            return jnp.einsum("td,tk->dk", rows, part, preferred_element_type=jnp.float32)

        return with_unit(coarse) + with_unit(fine)

    got = {}
    for flip in (3, 2, 1):
        got[flip] = to_peer(product(flip).astype(jnp.bfloat16), flip)
    got[0] = lax.optimization_barrier(product(0))

    chip = combined(rewards, filled, [got[flip] for flip in range(GROUP)], count)
    chip = chip.reshape(fsdp, rows_own, quarter)
    plane = lax.all_to_all(chip, FSDP, 0, 0, tiled=True)
    plane = plane.astype(jnp.float32).sum(axis=0)
    every = from_all(plane, REPLICA)
    every = every.reshape(replicas // GROUP, GROUP, rows_own, quarter).sum(axis=0)
    total = jnp.concatenate([every[k] for k in range(GROUP)], axis=-1) * grad_scale

    grad_weight = total * (1.0 + gain_own)[:, None]
    grad_gain = jnp.sum(total * kv_weight.astype(jnp.float32), axis=1)

    weights.append(to_peer(weights[0], 1))
    weights.append(to_peer(weights[0], 2))
    weights.append(to_peer(weights[2], 1))
    normed = (unit * (1.0 + gain_full)).astype(jnp.bfloat16)
    parts = [
        jnp.dot(normed, w, preferred_element_type=jnp.float32).astype(jnp.bfloat16) for w in weights
    ]
    placed = []
    for k in range(GROUP):
        chosen = parts[0]
        for flip in range(1, GROUP):
            chosen = jnp.where(place ^ flip == k, parts[flip], chosen)
        placed.append(chosen)
    key_values = jnp.concatenate(placed, axis=-1)
    return (key_values[None], grad_weight, grad_gain)


def solution(mesh):
    torus = Mesh(mesh.devices.reshape(8, 2, 8, 8), ALL)

    return jax.shard_map(
        shards,
        mesh=torus,
        in_specs=(
            P(ALL, None, None),
            P(ALL, None, None),
            P(FSDP, None),
            P(FSDP),
            P(ALL),
            P(ALL),
            P(ALL),
        ),
        out_specs=(P(ALL, None, None), P(FSDP, None), P(FSDP)),
        check_vma=False,
    )
```

```python
import functools

import jax
import jax.numpy as jnp
from jax import lax
from jax.experimental import pallas as pl
from jax.experimental.pallas import tpu as pltpu
from jax.sharding import Mesh
from jax.sharding import PartitionSpec as P

CORE, Z, X, Y = "core", "z", "x", "y"
REPLICA = (Z, CORE)
FSDP = (X, Y)
ALL = (Z, CORE, X, Y)
EPSILON = 1e-06
GROUP = 4
LANES = 128
DIGIT = 64.0
STEP = 4


def from_all(value, axes):
    count = lax.axis_size(axes)
    copies = jnp.broadcast_to(value[None], (count, *value.shape))
    return lax.all_to_all(copies, axes, 0, 0, tiled=True)


def to_peer(value, flip, upward=False):
    count = lax.axis_size(REPLICA)
    return lax.ppermute(value, REPLICA, [(i, peer_of(i, flip, upward, count)) for i in range(count)])


def peer_of(member, flip, upward, count):
    if upward and flip & 2:
        member = (member + (2 if member & 2 else -2)) % count
        return member ^ (flip & 1)
    return member ^ flip


def combine(count, rewards_ref, filled_ref, kept_ref, core_ref, *refs):
    *got_refs, out_ref = refs
    blocks, rows_own, _ = out_ref.shape
    half = rows_own // 2
    digits = filled_ref[:, rows_own:, :].astype(jnp.float32).sum(axis=0)
    sums = DIGIT * digits[1:2] + digits[2:3]
    average = sums[0, 0] / count
    scales = [rewards_ref[k] - average for k in range(6)]

    def block(step, carry):
        some = pl.ds(step * STEP, STEP)
        for upward in range(2):
            rows = pl.ds(upward * half, half)
            chip = scales[0] * kept_ref[some, rows, :]
            chip += scales[1] * core_ref[some, rows, :].astype(jnp.float32)
            for k in range(2):
                part = got_refs[2 * k + upward][some].astype(jnp.float32)
                chip += scales[2 + 2 * k + upward] * part
            out_ref[some, rows, :] = chip.astype(out_ref.dtype)
        return carry

    lax.fori_loop(0, blocks // STEP, block, 0)


def combined(rewards, filled, parts, count):
    shape = parts[0].shape
    vmem = pl.BlockSpec(memory_space=pltpu.VMEM)
    size = shape[0] * shape[1] * shape[2]
    return pl.pallas_call(
        functools.partial(combine, count),
        out_shape=jax.ShapeDtypeStruct(shape, jnp.bfloat16),
        in_specs=[pl.BlockSpec(memory_space=pltpu.SMEM), *([vmem] * (1 + len(parts)))],
        out_specs=vmem,
        compiler_params=pltpu.CompilerParams(vmem_limit_bytes=16 * 2**20),
        cost_estimate=pl.CostEstimate(flops=8 * size, bytes_accessed=12 * size, transcendentals=0),
        name="combine",
    )(rewards, filled, *parts)


def shards(states, cotangent, kv_weight, norm_gain, prompt_len, response_len, reward_bucket):
    fsdp, replicas = lax.axis_size(FSDP), lax.axis_size(REPLICA)
    member = lax.axis_index(REPLICA)
    place = member % GROUP
    rows_own, features = kv_weight.shape
    quarter = features // GROUP
    seq, width = states.shape[1:]

    def quarter_of(value, flip):
        return lax.dynamic_slice_in_dim(value, (place ^ flip) * quarter, quarter, value.ndim - 1)

    reward = reward_bucket.astype(jnp.float32)
    stats = jnp.concatenate([reward, reward * reward, response_len.astype(jnp.float32)])
    stats = from_all(jnp.pad(stats, (0, LANES - 3)), REPLICA)
    others = jnp.arange(replicas)
    rises = jnp.where(member & 2 == 0, member - 2, member + 2) % replicas
    peers = (member, member ^ 1, member ^ 2, rises, member ^ 3, rises ^ 1)
    rewards = jnp.stack([jnp.sum(jnp.where(others == k, stats[:, 0], 0.0)) for k in peers])
    sums = stats.sum(axis=0)
    high = jnp.floor(sums / DIGIT)
    low = sums - DIGIT * high
    extra = jnp.stack([jnp.pad(norm_gain, (0, LANES - rows_own)), high.astype(jnp.bfloat16), low.astype(jnp.bfloat16)])
    filled = from_all(jnp.concatenate([quarter_of(kv_weight, 0), extra]), FSDP)
    weights = [filled[:, :rows_own].reshape(width, quarter)]
    extra = filled[:, rows_own:].astype(jnp.float32)
    gain_own = norm_gain.astype(jnp.float32)
    gain_full = extra[:, 0, :rows_own].reshape(width)
    sums = jnp.sum(DIGIT * extra[:, 1] + extra[:, 2], axis=0)
    count = fsdp * replicas
    average = sums[0] / count
    variance = sums[1] / count - average * average
    grad_scale = lax.rsqrt(variance + EPSILON) * lax.rsqrt(sums[2])

    widened = states[0].astype(jnp.float32)
    mean = jnp.mean(widened * widened, axis=-1, keepdims=True)
    unit = widened * lax.rsqrt(mean + EPSILON)
    coarse = lax.reduce_precision(unit, 8, 7)
    fine = (unit - coarse).astype(jnp.bfloat16)
    coarse = coarse.astype(jnp.bfloat16)
    position = jnp.arange(seq, dtype=jnp.int32)
    live = (position >= prompt_len[0]) & (position < prompt_len[0] + response_len[0])
    masked = jnp.where(live[:, None], cotangent[0], jnp.zeros((), cotangent.dtype))

    def product(flip):
        def with_unit(rows):
            part = quarter_of(masked, flip)
            return jnp.einsum("td,tk->dk", rows, part, preferred_element_type=jnp.float32)

        return with_unit(coarse) + with_unit(fine)

    got = []
    for flip in (3, 2):
        made = product(flip).astype(jnp.bfloat16).reshape(fsdp, 2, rows_own // 2, quarter)
        halves = [made[:, 0], made[:, 1]]
        swapped = [to_peer(half, flip, upward=bool(k)) for k, half in enumerate(halves)]
        got = [*swapped, *got]
    blocks = (fsdp, rows_own, quarter)
    made = product(1).astype(jnp.bfloat16).reshape(blocks)
    across = to_peer(made, 1)
    kept = lax.optimization_barrier(product(0).reshape(blocks))

    chip = combined(rewards, filled, [kept, across, *got], count)
    plane = lax.all_to_all(chip, FSDP, 0, 0, tiled=True)
    plane = plane.astype(jnp.float32).sum(axis=0)
    every = from_all(plane, REPLICA)
    every = every.reshape(replicas // GROUP, GROUP, rows_own, quarter).sum(axis=0)
    total = jnp.concatenate([every[k] for k in range(GROUP)], axis=-1) * grad_scale

    grad_weight = total * (1.0 + gain_own)[:, None]
    grad_gain = jnp.sum(total * kv_weight.astype(jnp.float32), axis=1)

    weights.append(to_peer(weights[0], 1))
    weights.append(to_peer(weights[0], 2))
    weights.append(to_peer(weights[2], 1))
    normed = (unit * (1.0 + gain_full)).astype(jnp.bfloat16)
    parts = [
        jnp.dot(normed, w, preferred_element_type=jnp.float32).astype(jnp.bfloat16) for w in weights
    ]
    placed = []
    for k in range(GROUP):
        chosen = parts[0]
        for flip in range(1, GROUP):
            chosen = jnp.where(place ^ flip == k, parts[flip], chosen)
        placed.append(chosen)
    key_values = jnp.concatenate(placed, axis=-1)
    return (key_values[None], grad_weight, grad_gain)


def solution(mesh):
    torus = Mesh(mesh.devices.reshape(8, 2, 8, 8), ALL)

    return jax.shard_map(
        shards,
        mesh=torus,
        in_specs=(
            P(ALL, None, None),
            P(ALL, None, None),
            P(FSDP, None),
            P(FSDP),
            P(ALL),
            P(ALL),
            P(ALL),
        ),
        out_specs=(P(ALL, None, None), P(FSDP, None), P(FSDP)),
        check_vma=False,
    )
```

```python
import functools

import jax
import jax.numpy as jnp
from jax import lax
from jax.experimental import pallas as pl
from jax.experimental.pallas import tpu as pltpu
from jax.sharding import Mesh
from jax.sharding import PartitionSpec as P

CORE, Z, X, Y = "core", "z", "x", "y"
REPLICA = (Z, CORE)
FSDP = (X, Y)
ALL = (Z, CORE, X, Y)
EPSILON = 1e-06
GROUP = 4
LANES = 128
DIGIT = 64.0
STEP = 128


def from_all(value, axes):
    count = lax.axis_size(axes)
    copies = jnp.broadcast_to(value[None], (count, *value.shape))
    return lax.all_to_all(copies, axes, 0, 0, tiled=True)


def peer_of(member, peer, count):
    if peer == 3:
        return (member + (2 if member & 2 else -2)) % count ^ 1
    return member ^ peer


def to_peer(value, peer):
    count = lax.axis_size(REPLICA)
    return lax.ppermute(value, REPLICA, [(i, peer_of(i, peer, count)) for i in range(count)])


def combine(count, rewards_ref, filled_ref, *refs):
    *parts_refs, out_ref = refs
    width = out_ref.shape[0]
    extra_rows = filled_ref.shape[1] - 3
    digits = filled_ref[:, extra_rows:, :].astype(jnp.float32).sum(axis=0)
    sums = DIGIT * digits[1:2] + digits[2:3]
    average = sums[0, 0] / count
    scales = [rewards_ref[k] - average for k in range(GROUP)]

    def block(step, carry):
        rows = pl.ds(step * STEP, STEP)
        chip = scales[0] * parts_refs[0][rows, :]
        for peer in range(1, GROUP):
            chip += scales[peer] * parts_refs[peer][rows, :].astype(jnp.float32)
        out_ref[rows, :] = chip.astype(out_ref.dtype)
        return carry

    lax.fori_loop(0, width // STEP, block, 0)


def combined(rewards, filled, parts, count):
    width, quarter = parts[0].shape
    vmem = pl.BlockSpec(memory_space=pltpu.VMEM)
    return pl.pallas_call(
        functools.partial(combine, count),
        out_shape=jax.ShapeDtypeStruct((width, quarter), jnp.bfloat16),
        in_specs=[pl.BlockSpec(memory_space=pltpu.SMEM), *([vmem] * (1 + GROUP))],
        out_specs=vmem,
        compiler_params=pltpu.CompilerParams(vmem_limit_bytes=16 * 2**20),
        cost_estimate=pl.CostEstimate(
            flops=8 * width * quarter, bytes_accessed=12 * width * quarter, transcendentals=0
        ),
        name="combine",
    )(rewards, filled, *parts)


def shards(states, cotangent, kv_weight, norm_gain, prompt_len, response_len, reward_bucket):
    fsdp, replicas = lax.axis_size(FSDP), lax.axis_size(REPLICA)
    member = lax.axis_index(REPLICA)
    place = member % GROUP
    rows_own, features = kv_weight.shape
    quarter = features // GROUP
    seq, width = states.shape[1:]

    def quarter_of(value, flip):
        return lax.dynamic_slice_in_dim(value, (place ^ flip) * quarter, quarter, value.ndim - 1)

    reward = reward_bucket.astype(jnp.float32)
    stats = jnp.concatenate([reward, reward * reward, response_len.astype(jnp.float32)])
    stats = from_all(jnp.pad(stats, (0, LANES - 3)), REPLICA)
    above = jnp.where(member & 2 == 0, member - 2, member + 2) % replicas ^ 1
    which = jnp.arange(GROUP)
    peers = jnp.where(which == 3, above, member ^ which)
    chosen = peers[:, None] == jnp.arange(replicas)[None, :]
    rewards = jnp.sum(jnp.where(chosen, stats[:, 0][None, :], 0.0), axis=1)
    sums = stats.sum(axis=0)
    high = jnp.floor(sums / DIGIT)
    low = sums - DIGIT * high
    extra = jnp.stack([jnp.pad(norm_gain, (0, LANES - rows_own)), high.astype(jnp.bfloat16), low.astype(jnp.bfloat16)])
    filled = from_all(jnp.concatenate([quarter_of(kv_weight, 0), extra]), FSDP)
    weights = [filled[:, :rows_own].reshape(width, quarter)]
    extra = filled[:, rows_own:].astype(jnp.float32)
    gain_own = norm_gain.astype(jnp.float32)
    gain_full = extra[:, 0, :rows_own].reshape(width)
    sums = jnp.sum(DIGIT * extra[:, 1] + extra[:, 2], axis=0)
    count = fsdp * replicas
    average = sums[0] / count
    variance = sums[1] / count - average * average
    grad_scale = lax.rsqrt(variance + EPSILON) * lax.rsqrt(sums[2])

    widened = states[0].astype(jnp.float32)
    mean = jnp.mean(widened * widened, axis=-1, keepdims=True)
    unit = widened * lax.rsqrt(mean + EPSILON)
    coarse = lax.reduce_precision(unit, 8, 7)
    fine = (unit - coarse).astype(jnp.bfloat16)
    coarse = coarse.astype(jnp.bfloat16)
    position = jnp.arange(seq, dtype=jnp.int32)
    live = (position >= prompt_len[0]) & (position < prompt_len[0] + response_len[0])
    masked = jnp.where(live[:, None], cotangent[0], jnp.zeros((), cotangent.dtype))

    def product(flip):
        def with_unit(rows):
            part = quarter_of(masked, flip)
            return jnp.einsum("td,tk->dk", rows, part, preferred_element_type=jnp.float32)

        return with_unit(coarse) + with_unit(fine)

    parts = {}
    for peer in (3, 2, 1):
        made = product(peer).astype(jnp.bfloat16)
        parts[peer] = to_peer(made, peer)
    parts[0] = lax.optimization_barrier(product(0))

    chip = combined(rewards, filled, [parts[peer] for peer in range(GROUP)], count)
    chip = chip.reshape(fsdp, rows_own, quarter)
    plane = lax.all_to_all(chip, FSDP, 0, 0, tiled=True)
    plane = plane.astype(jnp.float32).sum(axis=0)
    every = from_all(plane, REPLICA)
    every = every.reshape(replicas // GROUP, GROUP, rows_own, quarter).sum(axis=0)
    total = jnp.concatenate([every[k] for k in range(GROUP)], axis=-1) * grad_scale

    grad_weight = total * (1.0 + gain_own)[:, None]
    grad_gain = jnp.sum(total * kv_weight.astype(jnp.float32), axis=1)

    weights.append(to_peer(weights[0], 1))
    weights.append(to_peer(weights[0], 2))
    weights.append(to_peer(weights[2], 1))
    normed = (unit * (1.0 + gain_full)).astype(jnp.bfloat16)
    parts = [
        jnp.dot(normed, w, preferred_element_type=jnp.float32).astype(jnp.bfloat16) for w in weights
    ]
    placed = []
    for k in range(GROUP):
        chosen = parts[0]
        for flip in range(1, GROUP):
            chosen = jnp.where(place ^ flip == k, parts[flip], chosen)
        placed.append(chosen)
    key_values = jnp.concatenate(placed, axis=-1)
    return (key_values[None], grad_weight, grad_gain)


def solution(mesh):
    torus = Mesh(mesh.devices.reshape(8, 2, 8, 8), ALL)

    return jax.shard_map(
        shards,
        mesh=torus,
        in_specs=(
            P(ALL, None, None),
            P(ALL, None, None),
            P(FSDP, None),
            P(FSDP),
            P(ALL),
            P(ALL),
            P(ALL),
        ),
        out_specs=(P(ALL, None, None), P(FSDP, None), P(FSDP)),
        check_vma=False,
    )
```

```python
import functools

import jax
import jax.numpy as jnp
from jax import lax
from jax.experimental import pallas as pl
from jax.experimental.pallas import tpu as pltpu
from jax.sharding import Mesh
from jax.sharding import PartitionSpec as P

CORE, Z, X, Y = "core", "z", "x", "y"
REPLICA = (Z, CORE)
FSDP = (X, Y)
ALL = (Z, CORE, X, Y)
EPSILON = 1e-06
GROUP = 4
LANES = 128
DIGIT = 64.0
STEP = 128


def from_all(value, axes):
    count = lax.axis_size(axes)
    copies = jnp.broadcast_to(value[None], (count, *value.shape))
    return lax.all_to_all(copies, axes, 0, 0, tiled=True)


def to_peer(value, flip):
    count = lax.axis_size(REPLICA)
    return lax.ppermute(value, REPLICA, [(i, i ^ flip) for i in range(count)])


def combine(count, rewards_ref, filled_ref, kept_ref, *refs):
    *got_refs, out_ref = refs
    width, _ = out_ref.shape
    extra_rows = filled_ref.shape[1] - 3
    digits = filled_ref[:, extra_rows:, :].astype(jnp.float32).sum(axis=0)
    sums = DIGIT * digits[1:2] + digits[2:3]
    average = sums[0, 0] / count
    scales = [rewards_ref[flip] - average for flip in range(GROUP)]

    def block(step, carry):
        rows = pl.ds(step * STEP, STEP)
        chip = scales[0] * kept_ref[rows, :]
        for flip in range(1, GROUP):
            chip += scales[flip] * got_refs[flip - 1][rows, :].astype(jnp.float32)
        out_ref[rows, :] = chip.astype(out_ref.dtype)
        return carry

    lax.fori_loop(0, width // STEP, block, 0)


def combined(rewards, filled, parts, count):
    width, quarter = parts[0].shape
    vmem = pl.BlockSpec(memory_space=pltpu.VMEM)
    return pl.pallas_call(
        functools.partial(combine, count),
        out_shape=jax.ShapeDtypeStruct((width, quarter), jnp.bfloat16),
        in_specs=[pl.BlockSpec(memory_space=pltpu.SMEM), *([vmem] * (1 + GROUP))],
        out_specs=vmem,
        compiler_params=pltpu.CompilerParams(vmem_limit_bytes=16 * 2**20),
        cost_estimate=pl.CostEstimate(
            flops=8 * width * quarter, bytes_accessed=12 * width * quarter, transcendentals=0
        ),
        name="combine",
    )(rewards, filled, *parts)


def shards(states, cotangent, kv_weight, norm_gain, prompt_len, response_len, reward_bucket):
    fsdp, replicas = lax.axis_size(FSDP), lax.axis_size(REPLICA)
    member = lax.axis_index(REPLICA)
    place = member % GROUP
    rows_own, features = kv_weight.shape
    quarter = features // GROUP
    seq, width = states.shape[1:]

    def quarter_of(value, flip):
        return lax.dynamic_slice_in_dim(value, (place ^ flip) * quarter, quarter, value.ndim - 1)

    reward = reward_bucket.astype(jnp.float32)
    lane = jnp.arange(LANES)
    stats = jnp.where(lane == 1, reward * reward, response_len.astype(jnp.float32))
    stats = jnp.where(lane == 0, reward, jnp.where(lane < 3, stats, 0.0))
    stats = from_all(stats, REPLICA)
    chosen = member ^ jnp.arange(GROUP)[:, None] == jnp.arange(replicas)[None, :]
    rewards = jnp.sum(jnp.where(chosen, stats[:, 0][None, :], 0.0), axis=1)
    sums = stats.sum(axis=0)
    high = jnp.floor(sums / DIGIT)
    low = sums - DIGIT * high
    extra = jnp.stack([jnp.pad(norm_gain, (0, LANES - rows_own)), high.astype(jnp.bfloat16), low.astype(jnp.bfloat16)])
    own = quarter_of(kv_weight, 0)
    filled = from_all(jnp.concatenate([own, extra]), FSDP)
    weights = [filled[:, :rows_own].reshape(width, quarter)]
    extra = filled[:, rows_own:].astype(jnp.float32)
    gain_own = norm_gain.astype(jnp.float32)
    gain_full = extra[:, 0, :rows_own].reshape(width)
    sums = jnp.sum(DIGIT * extra[:, 1] + extra[:, 2], axis=0)
    count = fsdp * replicas
    average = sums[0] / count
    variance = sums[1] / count - average * average
    grad_scale = lax.rsqrt(variance + EPSILON) * lax.rsqrt(sums[2])

    widened = states[0].astype(jnp.float32)
    mean = jnp.mean(widened * widened, axis=-1, keepdims=True)
    unit = widened * lax.rsqrt(mean + EPSILON)
    coarse = lax.reduce_precision(unit, 8, 7)
    fine = (unit - coarse).astype(jnp.bfloat16)
    coarse = coarse.astype(jnp.bfloat16)
    position = jnp.arange(seq, dtype=jnp.int32)
    live = (position >= prompt_len[0]) & (position < prompt_len[0] + response_len[0])

    def product(flip):
        def with_unit(rows):
            part = quarter_of(cotangent[0], flip)
            part = jnp.where(live[:, None], part, jnp.zeros((), part.dtype))
            return jnp.einsum("td,tk->dk", rows, part, preferred_element_type=jnp.float32)

        return with_unit(coarse) + with_unit(fine)

    got = {}
    for flip in (3, 2, 1):
        got[flip] = to_peer(product(flip).astype(jnp.bfloat16), flip)
    got[0] = lax.optimization_barrier(product(0))

    chip = combined(rewards, filled, [got[flip] for flip in range(GROUP)], count)
    chip = chip.reshape(fsdp, rows_own, quarter)
    plane = lax.all_to_all(chip, FSDP, 0, 0, tiled=True)
    plane = plane.astype(jnp.float32).sum(axis=0)
    every = from_all((plane * grad_scale).astype(jnp.bfloat16), REPLICA)
    every = every.astype(jnp.float32).reshape(replicas // GROUP, GROUP, rows_own, quarter).sum(axis=0)
    total = jnp.concatenate([every[k] for k in range(GROUP)], axis=-1)

    grad_weight = total * (1.0 + gain_own)[:, None]
    grad_gain = jnp.sum(total * kv_weight.astype(jnp.float32), axis=1)

    weights.append(to_peer(weights[0], 1))
    weights.append(to_peer(weights[0], 2))
    weights.append(to_peer(weights[2], 1))
    normed = (unit * (1.0 + gain_full)).astype(jnp.bfloat16)
    parts = [
        jnp.dot(normed, w, preferred_element_type=jnp.float32).astype(jnp.bfloat16) for w in weights
    ]
    placed = []
    for k in range(GROUP):
        chosen = parts[0]
        for flip in range(1, GROUP):
            chosen = jnp.where(place ^ flip == k, parts[flip], chosen)
        placed.append(chosen)
    key_values = jnp.concatenate(placed, axis=-1)
    return (key_values[None], grad_weight, grad_gain)


def solution(mesh):
    torus = Mesh(mesh.devices.reshape(8, 2, 8, 8), ALL)

    return jax.shard_map(
        shards,
        mesh=torus,
        in_specs=(
            P(ALL, None, None),
            P(ALL, None, None),
            P(FSDP, None),
            P(FSDP),
            P(ALL),
            P(ALL),
            P(ALL),
        ),
        out_specs=(P(ALL, None, None), P(FSDP, None), P(FSDP)),
        check_vma=False,
    )
```
